256 devices in a mesh: rows: 64 (over z, y, core), panel: 4 (over x).
Axes of the slice: x: 4, y: 4, z: 8, core: 2. Of those that a mesh axis runs over, the one named last changes fastest.
Arguments:
- pair_block: bfloat16 [2048, 16384], P('rows', 'panel'), may hold values from -6 to 6
- resolvent: float32 [16384, 16384], P('panel', 'rows'), may hold values from -0.046875 to 0.046875
- virt_coef: bfloat16 [1024, 11200], P('rows', 'panel'), may hold values from -0.1875 to 0.1875
- slot_row: int32 [2048], replicated, may hold values from 0 to 2047, each once
Outputs:
- backward: float32 [2, 11200, 16384], P(None, 'panel', 'rows')
The draws below stay inside these ranges and needn't reach their ends.
Inputs may be any that keep to these rules, and one draw needn't show every extreme that they name: `slot_row`: every pair row appears exactly once.
All inputs are finite; a program needn't handle non-finite values.
Results may differ from the reference program's by a relative error of at most 0.0041.
Values may be sent and summed in bfloat16 or wider, within the bound.
A program may use at most 128 MiB of HBM per device.

```python
import jax
import jax.numpy as jnp

NAUX = 16384
NAO = 11200
PAIRS = 2048
OCC_B = 2
VW = 1024


def levels(own_key, dims, pieces, smallest, top_value):
    loudness = 1.0
    for dim, shards_of in pieces:
        draws = jax.random.uniform(jax.random.fold_in(jax.random.fold_in(own_key, 6), dim), (shards_of,), jnp.float32, smallest / len(pieces), top_value / len(pieces))
        loudness = loudness * jnp.repeat(jnp.exp(draws), dims[dim] // shards_of).reshape((-1,) + (1,) * (len(dims) - 1 - dim))
    return loudness


def noise(stream_key, dims, deviation, limit, shards=(), kind=jnp.bfloat16):
    drawn = deviation * jax.random.normal(stream_key, dims, jnp.float32)
    if shards:
        drawn = drawn * levels(stream_key, dims, shards, -0.22, 0.18)
    return jnp.clip(drawn, -limit, limit).astype(kind)


def setup_inputs(seed: int = 0) -> dict:
    seeds = jax.random.split(jax.random.key(seed), 5)
    pair_block = noise(seeds[0], (PAIRS, NAUX), 1.0, 6.0, ((0, 64), (1, 4)))
    resolvent = noise(seeds[1], (NAUX, NAUX), NAUX ** -0.5, 0.046875, ((0, 4), (1, 64)), jnp.float32)
    virt_coef = noise(seeds[2], (VW, NAO), VW ** -0.5, 0.1875, ((0, 64), (1, 4)))
    slot_row = jax.random.permutation(seeds[3], PAIRS).astype(jnp.int32)
    return {"pair_block": pair_block, "resolvent": resolvent, "virt_coef": virt_coef, "slot_row": slot_row}


def reference(pair_block, resolvent, virt_coef, slot_row):
    resolvent_round = resolvent.astype(jnp.bfloat16)
    gamma = jnp.dot(pair_block, resolvent_round, preferred_element_type=jnp.float32)
    gamma_round = gamma.astype(jnp.bfloat16)
    grouped = jnp.take(gamma_round, slot_row.astype(jnp.int32), axis=0)
    grouped = grouped.reshape(OCC_B, PAIRS // OCC_B, gamma.shape[1])
    return jnp.einsum("am,oac->omc", virt_coef.astype(jnp.float32), grouped.astype(jnp.float32))
```

```python
import functools

import jax
import jax.numpy as jnp
from jax import lax
from jax.experimental import pallas as pl
from jax.experimental.pallas import tpu as pltpu
from jax.sharding import PartitionSpec as P

MESH = pl.DeviceIdType.MESH

NX, NY, NZ, NC = 4, 4, 8, 2
ROWS, KB, PB = 32, 4096, 256
CR, CM, CP = 16, 2800, 2816
KA, CA = 1664, 1152

ORDER = (
    (0, 1, 0), (0, 3, 0), (1, 0, 1), (1, 0, 7), (1, 1, 0), (1, 3, 0), (0, 0, 1), (0, 0, 7), (0, 2, 0), (0, 1, 1),
    (0, 1, 7), (1, 3, 1), (0, 3, 1), (0, 3, 7), (1, 1, 1), (1, 3, 7), (1, 1, 7), (1, 0, 2), (1, 0, 6), (1, 2, 0),
    (5, 0, 0), (0, 0, 2), (0, 0, 6), (1, 2, 1), (0, 2, 1), (0, 2, 7), (5, 1, 0), (1, 3, 2), (0, 1, 2), (0, 1, 6),
    (6, 0, 0), (1, 2, 7), (5, 7, 0), (1, 3, 6), (0, 3, 2), (0, 3, 6), (1, 1, 2), (6, 1, 0), (1, 1, 6), (1, 0, 3),
    (1, 0, 5), (7, 0, 0), (1, 2, 2), (6, 7, 0), (0, 0, 3), (0, 0, 5), (1, 2, 6), (0, 2, 2), (0, 2, 6), (5, 2, 0),
    (5, 6, 0), (1, 3, 3), (7, 1, 0), (7, 7, 0), (0, 1, 3), (0, 1, 5), (1, 1, 3), (1, 3, 5), (0, 3, 3), (0, 3, 5),
    (1, 1, 5), (6, 2, 0), (6, 6, 0), (1, 2, 3), (0, 2, 5), (4, 0, 0), (1, 0, 4), (0, 0, 4), (1, 2, 5), (5, 5, 0),
    (3, 1, 0), (3, 3, 0), (3, 0, 7), (0, 2, 3), (5, 3, 0), (2, 1, 0), (2, 3, 0), (2, 0, 7), (7, 2, 0), (7, 6, 0),
    (0, 1, 4), (3, 0, 6), (0, 3, 4), (2, 1, 7), (1, 1, 4), (1, 3, 4), (6, 5, 0), (2, 3, 7), (3, 0, 1), (3, 2, 0),
    (3, 3, 7), (2, 0, 6), (2, 0, 1), (3, 1, 7), (3, 3, 6), (6, 3, 0), (3, 0, 5), (2, 2, 0), (2, 1, 6), (3, 1, 6),
    (0, 2, 4), (3, 3, 1), (2, 3, 6), (2, 1, 1), (2, 0, 5), (8, 0, 0), (2, 3, 1), (3, 3, 5), (2, 2, 7), (1, 2, 4),
    (5, 4, 0), (2, 1, 5), (3, 1, 1), (3, 0, 2), (3, 2, 7), (2, 3, 5), (2, 0, 2), (7, 3, 0), (7, 5, 0), (3, 1, 5),
    (2, 2, 1), (3, 2, 6), (2, 2, 6), (2, 1, 2), (2, 3, 2), (3, 0, 3), (3, 2, 1), (3, 3, 2), (2, 0, 3), (2, 2, 2),
    (3, 1, 2), (3, 2, 5), (2, 2, 5), (2, 1, 3), (2, 3, 3), (6, 4, 0), (3, 0, 4), (8, 1, 0), (8, 7, 0), (2, 0, 4),
    (3, 1, 3), (3, 3, 3), (2, 2, 3), (3, 2, 2), (2, 1, 4), (2, 3, 4), (3, 1, 4), (3, 3, 4), (2, 2, 4), (8, 2, 0),
    (8, 6, 0), (3, 2, 3), (7, 4, 0), (3, 2, 4), (8, 3, 0), (8, 5, 0), (8, 4, 0),
)


def kernel(pair, res, coef, slots, ct, grouped, blocks, weights, stage, coefs, wide, parts, other, final, gamma, total,
           column, res_sem, block_sem, coef_sem, send_sem, half_sem, plane_sem):
    row, x = lax.axis_index("rows"), lax.axis_index("panel")
    core, y, z = row % NC, (row // NC) % NY, row // (NC * NY)
    turn = 1 - 2 * core
    mate = row + turn
    bf16, f32 = jnp.bfloat16, jnp.float32

    def at(dy, dz):
        return (y + NY - turn * dy) % NY, (z + NZ - turn * dz) % NZ

    def device(dy, dz):
        ty, tz = (y + NY + turn * dy) % NY, (z + NZ + turn * dz) % NZ
        return ((tz * NY + ty) * NC + core, x)

    def remote(src, dst, sent, got, to):
        return pltpu.make_async_remote_copy(
            src_ref=src, dst_ref=dst, send_sem=sent, recv_sem=got, device_id=to, device_id_type=MESH
        )

    step = KB // 4
    loads = [
        pltpu.make_async_copy(res.at[pl.ds(i * step, step)], stage.at[pl.ds(i * step, step)], res_sem.at[i])
        for i in range(4)
    ]
    for load in loads:
        load.start()

    barrier = pltpu.get_barrier_semaphore()
    peers = [device(1, 0), device(-1, 0), device(0, 1), device(0, -1), (mate, x)]
    peers += [(r, (x + d) % NX) for d in range(1, NX) for r in (row, mate)]
    for peer in peers:
        pl.semaphore_signal(barrier, inc=1, device_id=peer, device_id_type=MESH)
    pl.semaphore_wait(barrier, len(peers))

    def piece(kind, place):
        chip, plane = place[1] * NY + place[0], None
        if kind < 2:
            return blocks.at[chip, :, pl.ds(0, KA) if kind == 0 else pl.ds(KA, KB - KA)]
        return coefs.at[chip * NC + core, :, pl.ds(0, CA) if kind == 2 else pl.ds(CA, CP - CA)]

    def arrival(kind, place):
        sems = block_sem if kind < 2 else coef_sem
        return sems.at[kind % 2, place[1] * NY + place[0]]

    def pass_on(kind, dy, dz):
        place = at(dy, dz)
        ref = piece(kind, place)
        src = ref
        if kind < 2 and dy == 0 and dz == 0:
            src = pair.at[:, pl.ds(0, KA) if kind == 0 else pl.ds(KA, KB - KA)]
        along_y = []
        along_z = []
        if kind % 2 == 0:
            if dz == 0:
                along_y = [1] * (dy in (0, 1)) + [-1] * (dy == 0)
                along_z = [1, -1]
            else:
                along_z = [1] * (dz in (1, 2, 3)) + [-1] * (dz in (6, 7))
        else:
            if dy == 0:
                along_z = [1] * (dz in (0, 1, 2, 3)) + [-1] * (dz in (0, 6, 7))
                along_y = [1, -1]
            elif dy == 1:
                along_y = [1]
        hops = [(d, 0) for d in along_y] + [(0, d) for d in along_z]
        for hop in hops:
            remote(src, ref, send_sem.at[kind], arrival(kind, place), device(*hop)).start()

    pass_on(0, 0, 0)
    pass_on(1, 0, 0)

    chip = z * NY + y
    blocks[chip] = pair[...]
    own = coef[...]
    coefs[row] = jnp.concatenate([own, jnp.zeros((CR, CP - CM), bf16)], axis=1)
    for i in range(16):
        wide_row = jnp.broadcast_to(slots[i : i + 1, :].astype(f32), (128, 128))
        column[pl.ds(i * 128, 128), :] = jnp.transpose(wide_row).astype(jnp.int32)
    total[...] = jnp.zeros_like(total)
    for i in range(5):
        if i < 4:
            loads[i].wait()
            weights[core, pl.ds(i * step, step), :] = stage[pl.ds(i * step, step), :].astype(bf16)
        if i > 0:
            ref = weights.at[core, pl.ds((i - 1) * step, step)]
            remote(ref, ref, half_sem.at[0], half_sem.at[1], (mate, x)).start()
    whole = weights.at[1 - core]
    remote(whole, whole, half_sem.at[0], half_sem.at[1], (mate, x)).wait_recv()

    def share_coefs(place):
        ref = coefs.at[(place[1] * NY + place[0]) * NC + core]
        remote(ref, ref, send_sem.at[4], plane_sem.at[2, place[1]], (mate, x)).start()

    def multiply(dz):
        _, plane = at(0, dz)
        first = plane * NY
        for half in range(NC):
            def over(k, carry):
                cols = pl.ds(pl.multiple_of(k * 1024, 1024), 1024)
                left = blocks[pl.ds(first, NY), :, cols].reshape(NY * ROWS, 1024)
                prod = jnp.dot(left, weights[half, cols, :], preferred_element_type=f32)
                return carry + prod
            prod = lax.fori_loop(0, 4, over, jnp.zeros((NY * ROWS, PB), f32)).reshape(NY, ROWS, PB)
            wide[plane, :, half] = prod
            parts[plane, :, half] = prod.astype(bf16)
        for d in range(1, NX):
            to = (x + d) % NX
            remote(parts.at[plane, to], other.at[plane, d - 1], send_sem.at[5], plane_sem.at[0, plane], (row, to)).start()

    def add_up(dz):
        _, plane = at(0, dz)
        ref = other.at[plane]
        remote(ref, ref, send_sem.at[5], plane_sem.at[0, plane], (row, x)).wait_recv()
        value = wide[plane, x]
        for d in range(NX - 1):
            value = value + other[plane, d].astype(f32)
        value = value.astype(bf16)
        final[plane] = value
        spot = plane * (NY * NC) + x * NC + core
        gamma[spot] = final[plane, core]
        remote(final.at[plane, 1 - core], gamma.at[spot], send_sem.at[6], plane_sem.at[1, plane], (mate, x)).start()
        for d in range(1, NX):
            for c in range(NC):
                to = ((z * NY + y) * NC + c, (x + d) % NX)
                remote(final.at[plane, c], gamma.at[spot], send_sem.at[6], plane_sem.at[1, plane], to).start()

    def select(dz):
        _, plane = at(0, dz)
        ref = gamma.at[pl.ds(0, NY * NC - 1)]
        remote(ref, ref, send_sem.at[6], plane_sem.at[1, plane], (mate, x)).wait_recv()
        rows = gamma[pl.ds(plane * (NY * NC), NY * NC)].reshape(NY * NC * ROWS, PB)
        base = plane * (NY * NC * ROWS)
        lanes = lax.broadcasted_iota(jnp.int32, (256, 128), 1)

        def over(i, carry):
            at_rows = pl.ds(pl.multiple_of(i * 256, 256), 256)
            ids = column[at_rows, :] - base
            pick = jnp.concatenate(
                [jnp.where(ids == lanes + h * 128, 1.0, 0.0).astype(bf16) for h in range(2)], axis=1
            )
            total[at_rows, :] += jnp.dot(pick, rows, preferred_element_type=f32)
            return carry

        lax.fori_loop(0, 8, over, 0)

    def transpose(dz):
        _, plane = at(0, dz)
        ref = coefs.at[pl.ds(0, NY)]
        remote(ref, ref, send_sem.at[4], plane_sem.at[2, plane], (mate, x)).wait_recv()
        out_cols = pl.ds(pl.multiple_of(plane * 128, 128), 128)

        def over(i, carry):
            cols = pl.ds(pl.multiple_of(i * 1408, 128), 1408)
            tile = coefs[pl.ds(plane * (NY * NC), NY * NC), :, cols].reshape(128, 1408)
            ct[cols, out_cols] = jnp.transpose(tile)
            return carry

        lax.fori_loop(0, 2, over, 0)

    seen = {}
    for kind, dy, dz in ORDER:
        if kind < 4:
            place = at(dy, dz)
            ref = piece(kind, place)
            remote(ref, ref, send_sem.at[kind], arrival(kind, place), (mate, x)).wait_recv()
            pass_on(kind, dy, dz)
            if kind >= 2:
                seen[dy, dz] = seen.get((dy, dz), 0) + 1
                if seen[dy, dz] == 2:
                    share_coefs(place)
        elif kind == 4:
            pass_on(3, 0, 0)
            pass_on(2, 0, 0)
            share_coefs(at(0, 0))
        else:
            {5: multiply, 6: add_up, 7: select, 8: transpose}[kind](dy)

    grouped[...] = total[...].astype(bf16)

    def drained(ref, sem):
        remote(ref, ref, sem, half_sem.at[1], (mate, x)).wait_send()

    sends = NY * NZ - 1
    drained(blocks.at[pl.ds(0, sends), :, pl.ds(0, KA)], send_sem.at[0])
    drained(blocks.at[pl.ds(0, sends), :, pl.ds(KA, KB - KA)], send_sem.at[1])
    drained(coefs.at[pl.ds(0, sends), :, pl.ds(0, CA)], send_sem.at[2])
    drained(coefs.at[pl.ds(0, sends), :, pl.ds(CA, CP - CA)], send_sem.at[3])
    drained(coefs.at[pl.ds(0, NY * NZ)], send_sem.at[4])
    drained(other, send_sem.at[5])
    drained(gamma.at[pl.ds(0, NZ * (NY * NC - 1))], send_sem.at[6])
    drained(whole, half_sem.at[0])


def finish(ct, grouped, out):
    out[0] = jnp.dot(ct[...], grouped[...], preferred_element_type=jnp.float32)


def body(pair_block, resolvent, virt_coef, slot_row):
    vmem = pl.BlockSpec(memory_space=pltpu.VMEM)
    dma = pltpu.SemaphoreType.DMA
    bf16, f32 = jnp.bfloat16, jnp.float32
    ct, grouped = pl.pallas_call(
        kernel,
        out_shape=(
            jax.ShapeDtypeStruct((CP, NZ * NY * NC * CR), bf16),
            jax.ShapeDtypeStruct((NZ * NY * NC * ROWS, PB), bf16),
        ),
        in_specs=[vmem, pl.BlockSpec(memory_space=pl.ANY), vmem, vmem],
        out_specs=(vmem, vmem),
        scratch_shapes=[
            pltpu.VMEM((NY * NZ, ROWS, KB), bf16),
            pltpu.VMEM((NC, KB, PB), bf16),
            pltpu.VMEM((KB, PB), f32),
            pltpu.VMEM((NY * NZ * NC, CR, CP), bf16),
            pltpu.VMEM((NZ, NY, NC, ROWS, PB), f32),
            pltpu.VMEM((NZ, NY, NC, ROWS, PB), bf16),
            pltpu.VMEM((NZ, NX - 1, NC, ROWS, PB), bf16),
            pltpu.VMEM((NZ, NC, ROWS, PB), bf16),
            pltpu.VMEM((NZ * NY * NC, ROWS, PB), bf16),
            pltpu.VMEM((NZ * NY * NC * ROWS, PB), f32),
            pltpu.VMEM((NZ * NY * NC * ROWS, 128), jnp.int32),
            dma((4,)),
            dma((2, NY * NZ)),
            dma((2, NY * NZ)),
            dma((7,)),
            dma((2,)),
            dma((3, NZ)),
        ],
        compiler_params=pltpu.CompilerParams(
            collective_id=0, has_side_effects=True, vmem_limit_bytes=46 * 1024 * 1024
        ),
    )(pair_block, resolvent, virt_coef, slot_row.reshape(16, 128))
    width = NZ * NY * NC * CR
    tall = 400
    return pl.pallas_call(
        finish,
        grid=(CM // tall, 2),
        out_shape=jax.ShapeDtypeStruct((2, CM, PB), f32),
        in_specs=[
            pl.BlockSpec((tall, width), lambda i, o: (i, 0)),
            pl.BlockSpec((width, PB), lambda i, o: (o, 0)),
        ],
        out_specs=pl.BlockSpec((1, tall, PB), lambda i, o: (o, i, 0)),
        compiler_params=pltpu.CompilerParams(vmem_limit_bytes=16 * 1024 * 1024),
        cost_estimate=pl.CostEstimate(flops=4 * CM * width * PB, bytes_accessed=12000000, transcendentals=0),
    )(ct, grouped)


def solution(mesh):
    placed = (P("rows", "panel"), P("panel", "rows"), P("rows", "panel"), P())
    return jax.shard_map(
        body, mesh=mesh, in_specs=placed, out_specs=P(None, "panel", "rows"), check_vma=False
    )
```

```python
import functools

import jax
import jax.numpy as jnp
from jax import lax
from jax.experimental import pallas as pl
from jax.experimental.pallas import tpu as pltpu
from jax.sharding import PartitionSpec as P

MESH = pl.DeviceIdType.MESH

NX, NY, NZ, NC = 4, 4, 8, 2
ROWS, KB, PB = 32, 4096, 256
CHUNKS = 7
CR, CM, CP = 16, 2800, 2816
KA, CA = 1664, 1152

ORDER = (
    (9, 0, 0), (9, 1, 0), (9, 2, 0), (9, 3, 0), (9, 4, 0), (9, 5, 0), (0, 1, 0), (0, 3, 0), (0, 0, 1), (0, 0, 7),
    (1, 1, 0), (1, 3, 0), (1, 0, 1), (1, 0, 7), (0, 2, 0), (0, 1, 1), (0, 1, 7), (0, 3, 1), (0, 3, 7), (1, 2, 0),
    (5, 0, 0), (1, 3, 1), (5, 0, 1), (0, 0, 2), (0, 0, 6), (1, 1, 1), (1, 3, 7), (6, 0, 0), (1, 1, 7), (1, 0, 2),
    (1, 0, 6), (1, 2, 1), (0, 2, 1), (0, 2, 7), (5, 1, 0), (5, 1, 1), (7, 0, 0), (7, 0, 1), (0, 1, 2), (0, 1, 6),
    (1, 2, 7), (5, 7, 0), (1, 3, 2), (5, 7, 1), (6, 1, 0), (0, 3, 2), (0, 3, 6), (1, 1, 2), (1, 3, 6), (0, 0, 3),
    (0, 0, 5), (6, 7, 0), (1, 1, 6), (1, 2, 2), (1, 0, 3), (1, 0, 5), (7, 1, 0), (1, 2, 6), (7, 1, 1), (7, 7, 0),
    (7, 7, 1), (0, 2, 2), (0, 2, 6), (5, 2, 0), (5, 2, 1), (5, 6, 0), (5, 6, 1), (0, 1, 3), (0, 1, 5), (1, 1, 3),
    (1, 3, 3), (6, 2, 0), (0, 3, 3), (0, 3, 5), (6, 6, 0), (1, 1, 5), (1, 3, 5), (4, 0, 0), (0, 0, 4), (0, 2, 5),
    (1, 2, 3), (1, 0, 4), (7, 2, 0), (3, 3, 0), (3, 0, 7), (7, 2, 1), (7, 6, 0), (2, 3, 0), (2, 0, 7), (1, 2, 5),
    (0, 2, 3), (5, 3, 0), (5, 3, 1), (3, 1, 0), (5, 5, 0), (0, 1, 4), (5, 5, 1), (2, 1, 0), (3, 0, 6), (7, 6, 1),
    (2, 3, 7), (1, 3, 4), (2, 0, 6), (0, 3, 4), (6, 3, 0), (3, 3, 7), (3, 0, 1), (2, 1, 7), (1, 1, 4), (6, 5, 0),
    (2, 0, 1), (3, 3, 6), (3, 1, 7), (3, 0, 5), (2, 3, 1), (3, 2, 0), (2, 3, 6), (2, 2, 0), (3, 3, 1), (2, 0, 5),
    (3, 1, 6), (0, 2, 4), (2, 1, 6), (3, 3, 5), (8, 0, 0), (3, 1, 1), (2, 1, 1), (2, 3, 5), (8, 0, 1), (7, 3, 0),
    (7, 3, 1), (2, 2, 7), (3, 0, 2), (7, 5, 0), (1, 2, 4), (5, 4, 0), (2, 1, 5), (2, 0, 2), (3, 2, 7), (2, 3, 2),
    (3, 1, 5), (2, 2, 1), (5, 4, 1), (2, 1, 2), (3, 2, 6), (7, 5, 1), (2, 2, 6), (3, 0, 3), (3, 3, 2), (3, 2, 1),
    (2, 0, 3), (3, 1, 2), (2, 3, 3), (2, 2, 2), (3, 2, 5), (8, 1, 0), (2, 1, 3), (8, 1, 1), (2, 2, 5), (6, 4, 0),
    (3, 0, 4), (3, 1, 3), (3, 3, 3), (2, 0, 4), (8, 7, 0), (3, 2, 2), (2, 3, 4), (8, 7, 1), (2, 2, 3), (2, 1, 4),
    (8, 2, 0), (8, 2, 1), (8, 6, 0), (3, 1, 4), (3, 3, 4), (8, 6, 1), (2, 2, 4), (3, 2, 3), (7, 4, 0), (7, 4, 1),
    (10, 0, 0), (8, 3, 0), (3, 2, 4), (8, 3, 1), (8, 5, 0), (8, 5, 1), (8, 4, 0), (8, 4, 1),
)


def kernel(pair, res, coef, slots, ct, grouped, blocks, weights, stage, coefs, wide, parts, other, final, gamma, total,
           column, own_coef, own_slots, turned, rounded, load_sem, out_sem, block_sem, coef_sem, send_sem, half_sem,
           plane_sem):
    row, x = lax.axis_index("rows"), lax.axis_index("panel")
    core, y, z = row % NC, (row // NC) % NY, row // (NC * NY)
    turn = 1 - 2 * core
    mate = row + turn
    bf16, f32 = jnp.bfloat16, jnp.float32

    def at(dy, dz):
        return (y + NY - turn * dy) % NY, (z + NZ - turn * dz) % NZ

    def device(dy, dz):
        ty, tz = (y + NY + turn * dy) % NY, (z + NZ + turn * dz) % NZ
        return ((tz * NY + ty) * NC + core, x)

    def remote(src, dst, sent, got, to):
        return pltpu.make_async_remote_copy(
            src_ref=src, dst_ref=dst, send_sem=sent, recv_sem=got, device_id=to, device_id_type=MESH
        )

    own = z * NY + y
    step = KB // 4
    load_pair = pltpu.make_async_copy(pair, blocks.at[own], load_sem.at[4])
    load_pair.start()
    loads = [
        pltpu.make_async_copy(res.at[pl.ds(i * step, step)], stage.at[pl.ds(i * step, step)], load_sem.at[i])
        for i in range(4)
    ]
    load_coef = pltpu.make_async_copy(coef, own_coef, load_sem.at[5])
    load_slots = pltpu.make_async_copy(slots, own_slots, load_sem.at[6])
    for load in loads + [load_coef, load_slots]:
        load.start()

    barrier = pltpu.get_barrier_semaphore()
    peers = [device(1, 0), device(-1, 0), device(0, 1), device(0, -1), (mate, x)]
    peers += [(r, (x + d) % NX) for d in range(1, NX) for r in (row, mate)]
    for peer in peers:
        pl.semaphore_signal(barrier, inc=1, device_id=peer, device_id_type=MESH)
    load_pair.wait()
    pl.semaphore_wait(barrier, len(peers))

    def piece(kind, place):
        chip = place[1] * NY + place[0]
        if kind < 2:
            return blocks.at[chip, :, pl.ds(0, KA) if kind == 0 else pl.ds(KA, KB - KA)]
        return coefs.at[chip * NC + core, :, pl.ds(0, CA) if kind == 2 else pl.ds(CA, CP - CA)]

    def arrival(kind, place):
        sems = block_sem if kind < 2 else coef_sem
        return sems.at[kind % 2, place[1] * NY + place[0]]

    def pass_on(kind, dy, dz):
        place = at(dy, dz)
        ref = piece(kind, place)
        along_y = []
        along_z = []
        if kind % 2 == 0:
            if dz == 0:
                along_y = [1] * (dy in (0, 1)) + [-1] * (dy == 0)
                along_z = [1, -1]
            else:
                along_z = [1] * (dz in (1, 2, 3)) + [-1] * (dz in (6, 7))
        else:
            if dy == 0:
                along_z = [1] * (dz in (0, 1, 2, 3)) + [-1] * (dz in (0, 6, 7))
                along_y = [1, -1]
            elif dy == 1:
                along_y = [1]
        for hop in [(d, 0) for d in along_y] + [(0, d) for d in along_z]:
            remote(ref, ref, send_sem.at[kind], arrival(kind, place), device(*hop)).start()

    def share_coefs(place):
        ref = coefs.at[(place[1] * NY + place[0]) * NC + core]
        remote(ref, ref, send_sem.at[4], plane_sem.at[2, place[1]], (mate, x)).start()

    whole = weights.at[1 - core]

    def prepare(i, _):
        if i < 4:
            loads[i].wait()
            weights[core, pl.ds(i * step, step), :] = stage[pl.ds(i * step, step), :].astype(bf16)
        if 0 < i < 5:
            ref = weights.at[core, pl.ds((i - 1) * step, step)]
            remote(ref, ref, half_sem.at[0], half_sem.at[1], (mate, x)).start()
        if i == 5:
            load_coef.wait()
            coefs[row] = jnp.concatenate([own_coef[...], jnp.zeros((CR, CP - CM), bf16)], axis=1)
            load_slots.wait()
            for j in range(16):
                wide_row = jnp.broadcast_to(own_slots[j : j + 1, :].astype(f32), (128, 128))
                column[pl.ds(j * 128, 128), :] = jnp.transpose(wide_row).astype(jnp.int32)

    multiplied = set()

    def multiply(dz, half):
        if not multiplied:
            remote(whole, whole, half_sem.at[0], half_sem.at[1], (mate, x)).wait_recv()
        multiplied.add((dz, half))
        _, plane = at(0, dz)
        left = blocks[pl.ds(plane * NY, NY)].reshape(NY * ROWS, KB)
        prod = jnp.dot(left, weights[half], preferred_element_type=f32).reshape(NY, ROWS, PB)
        wide[plane, :, half] = prod
        parts[plane, :, half] = prod.astype(bf16)
        if half == NC - 1:
            for d in range(1, NX):
                to = (x + d) % NX
                ref = other.at[plane, d - 1]
                remote(parts.at[plane, to], ref, send_sem.at[5], plane_sem.at[0, plane], (row, to)).start()

    def add_up(dz, _):
        _, plane = at(0, dz)
        ref = other.at[plane]
        remote(ref, ref, send_sem.at[5], plane_sem.at[0, plane], (row, x)).wait_recv()
        value = wide[plane, x]
        for d in range(NX - 1):
            value = value + other[plane, d].astype(f32)
        final[plane] = value.astype(bf16)
        spot = plane * (NY * NC) + x * NC + core
        gamma[spot] = final[plane, core]
        remote(final.at[plane, 1 - core], gamma.at[spot], send_sem.at[6], plane_sem.at[1, plane], (mate, x)).start()
        for d in range(1, NX):
            for c in range(NC):
                to = ((z * NY + y) * NC + c, (x + d) % NX)
                remote(final.at[plane, c], gamma.at[spot], send_sem.at[6], plane_sem.at[1, plane], to).start()

    selected = set()

    def select(dz, part):
        _, plane = at(0, dz)
        if part == 0:
            ref = gamma.at[pl.ds(0, NY * NC - 1)]
            remote(ref, ref, send_sem.at[6], plane_sem.at[1, plane], (mate, x)).wait_recv()
        rows = gamma[pl.ds(plane * (NY * NC), NY * NC)].reshape(NY * NC * ROWS, PB)
        lanes = lax.broadcasted_iota(jnp.int32, (1024, 128), 1)
        at_rows = pl.ds(part * 1024, 1024)
        ids = column[at_rows, :] - plane * (NY * NC * ROWS)
        pick = jnp.concatenate(
            [jnp.where(ids == lanes + h * 128, 1.0, 0.0).astype(bf16) for h in range(2)], axis=1
        )
        found = jnp.dot(pick, rows, preferred_element_type=f32)
        if part in selected:
            found = total[at_rows, :] + found
        selected.add(part)
        total[at_rows, :] = found

    def transpose(dz, part):
        _, plane = at(0, dz)
        if part == 0:
            ref = coefs.at[pl.ds(0, NY)]
            remote(ref, ref, send_sem.at[4], plane_sem.at[2, plane], (mate, x)).wait_recv()
        cols = pl.ds(part * 1408, 1408)
        tile = coefs[pl.ds(plane * (NY * NC), NY * NC), :, cols].reshape(128, 1408)
        turned[plane, cols] = jnp.transpose(tile)
        pltpu.make_async_copy(turned.at[plane, cols], ct.at[plane, cols], out_sem.at[0]).start()

    hand_over = pltpu.make_async_copy(rounded, grouped, out_sem.at[1])

    def deliver(_, __):
        rounded[...] = total[...].astype(bf16)
        hand_over.start()

    pass_on(0, 0, 0)
    pass_on(1, 0, 0)
    seen = {}
    for kind, dy, dz in ORDER:
        if kind < 4:
            place = at(dy, dz)
            ref = piece(kind, place)
            remote(ref, ref, send_sem.at[kind], arrival(kind, place), (mate, x)).wait_recv()
            pass_on(kind, dy, dz)
            if kind >= 2:
                seen[dy, dz] = seen.get((dy, dz), 0) + 1
                if seen[dy, dz] == 2:
                    share_coefs(place)
        elif kind == 4:
            pass_on(3, 0, 0)
            pass_on(2, 0, 0)
            share_coefs(at(0, 0))
        else:
            {5: multiply, 6: add_up, 7: select, 8: transpose, 9: prepare, 10: deliver}[kind](dy, dz)

    def drained(ref, sem):
        remote(ref, ref, sem, half_sem.at[1], (mate, x)).wait_send()

    sends = NY * NZ - 1
    drained(blocks.at[pl.ds(0, sends), :, pl.ds(0, KA)], send_sem.at[0])
    drained(blocks.at[pl.ds(0, sends), :, pl.ds(KA, KB - KA)], send_sem.at[1])
    drained(coefs.at[pl.ds(0, sends), :, pl.ds(0, CA)], send_sem.at[2])
    drained(coefs.at[pl.ds(0, sends), :, pl.ds(CA, CP - CA)], send_sem.at[3])
    drained(coefs.at[pl.ds(0, NY * NZ)], send_sem.at[4])
    drained(other, send_sem.at[5])
    drained(gamma.at[pl.ds(0, NZ * (NY * NC - 1))], send_sem.at[6])
    drained(whole, half_sem.at[0])
    hand_over.wait()
    pltpu.make_async_copy(turned, ct, out_sem.at[0]).wait()


def finish(ct, grouped, out, left, right, result, left_sem, right_sem, result_sem):
    tall = CM // CHUNKS
    half = NZ * NY * NC * CR
    get_right = pltpu.make_async_copy(grouped, right, right_sem)
    get_right.start()
    gets = []
    for i in range(CHUNKS):
        rows = pl.ds(i * tall, tall)
        gets.append(pltpu.make_async_copy(ct.at[:, rows], left.at[:, rows], left_sem.at[i]))
        gets[i].start()
    get_right.wait()
    puts = []
    for i in range(CHUNKS):
        rows = pl.ds(i * tall, tall)
        gets[i].wait()
        tile = jnp.concatenate([left[plane, rows] for plane in range(NZ)], axis=1)
        for o in range(2):
            result[o, rows] = jnp.dot(tile, right[pl.ds(o * half, half)], preferred_element_type=jnp.float32)
        puts.append(pltpu.make_async_copy(result.at[:, rows], out.at[:, rows], result_sem.at[i]))
        puts[i].start()
    for put in puts:
        put.wait()


def body(pair_block, resolvent, virt_coef, slot_row):
    dma = pltpu.SemaphoreType.DMA
    bf16, f32 = jnp.bfloat16, jnp.float32
    anywhere = pl.BlockSpec(memory_space=pl.ANY)
    width = NY * NC * CR
    tall = NZ * NY * NC * ROWS
    ct, grouped = pl.pallas_call(
        kernel,
        out_shape=(jax.ShapeDtypeStruct((NZ, CP, width), bf16), jax.ShapeDtypeStruct((tall, PB), bf16)),
        in_specs=[anywhere] * 4,
        out_specs=(anywhere, anywhere),
        scratch_shapes=[
            pltpu.VMEM((NY * NZ, ROWS, KB), bf16),
            pltpu.VMEM((NC, KB, PB), bf16),
            pltpu.VMEM((KB, PB), f32),
            pltpu.VMEM((NY * NZ * NC, CR, CP), bf16),
            pltpu.VMEM((NZ, NY, NC, ROWS, PB), f32),
            pltpu.VMEM((NZ, NY, NC, ROWS, PB), bf16),
            pltpu.VMEM((NZ, NX - 1, NC, ROWS, PB), bf16),
            pltpu.VMEM((NZ, NC, ROWS, PB), bf16),
            pltpu.VMEM((NZ * NY * NC, ROWS, PB), bf16),
            pltpu.VMEM((tall, PB), f32),
            pltpu.VMEM((tall, 128), jnp.int32),
            pltpu.VMEM((CR, CM), bf16),
            pltpu.VMEM((16, 128), jnp.int32),
            pltpu.VMEM((NZ, CP, width), bf16),
            pltpu.VMEM((tall, PB), bf16),
            dma((7,)),
            dma((2,)),
            dma((2, NY * NZ)),
            dma((2, NY * NZ)),
            dma((7,)),
            dma((2,)),
            dma((3, NZ)),
        ],
        compiler_params=pltpu.CompilerParams(
            collective_id=0, has_side_effects=True, vmem_limit_bytes=60 * 1024 * 1024
        ),
    )(pair_block, resolvent, virt_coef, slot_row.reshape(16, 128))
    return pl.pallas_call(
        finish,
        out_shape=jax.ShapeDtypeStruct((2, CM, PB), f32),
        in_specs=[anywhere, anywhere],
        out_specs=anywhere,
        scratch_shapes=[
            pltpu.VMEM((NZ, CP, width), bf16),
            pltpu.VMEM((tall, PB), bf16),
            pltpu.VMEM((2, CM, PB), f32),
            dma((CHUNKS,)),
            dma,
            dma((CHUNKS,)),
        ],
        compiler_params=pltpu.CompilerParams(vmem_limit_bytes=60 * 1024 * 1024),
        cost_estimate=pl.CostEstimate(flops=4 * CM * NZ * width * PB, bytes_accessed=12000000, transcendentals=0),
    )(ct, grouped)


def solution(mesh):
    placed = (P("rows", "panel"), P("panel", "rows"), P("rows", "panel"), P())
    return jax.shard_map(
        body, mesh=mesh, in_specs=placed, out_specs=P(None, "panel", "rows"), check_vma=False
    )
```

```python
import functools

import jax
import jax.numpy as jnp
from jax import lax
from jax.experimental import pallas as pl
from jax.experimental.pallas import tpu as pltpu
from jax.sharding import PartitionSpec as P

MESH = pl.DeviceIdType.MESH

NX, NY, NZ, NC = 4, 4, 8, 2
ROWS, KB, PB = 32, 4096, 256
CHUNKS = 7
CR, CM, CP = 16, 2800, 2816
KA, CA = 1664, 1152

ORDER = (
    (9, 0, 0), (9, 1, 0), (9, 2, 0), (9, 3, 0), (9, 4, 0), (9, 5, 0), (0, 1, 0), (0, 3, 0), (0, 0, 1), (0, 0, 7),
    (1, 1, 0), (1, 3, 0), (1, 0, 1), (1, 0, 7), (0, 2, 0), (0, 1, 1), (0, 1, 7), (0, 3, 1), (0, 3, 7), (1, 2, 0),
    (5, 0, 0), (1, 3, 1), (5, 0, 1), (0, 0, 2), (0, 0, 6), (1, 1, 1), (1, 3, 7), (1, 0, 2), (1, 0, 6), (1, 1, 7),
    (6, 0, 0), (1, 2, 1), (0, 2, 1), (0, 2, 7), (5, 1, 0), (5, 1, 1), (0, 1, 2), (0, 1, 6), (1, 1, 2), (1, 3, 2),
    (7, 0, 0), (0, 3, 2), (0, 3, 6), (7, 0, 1), (1, 1, 6), (1, 3, 6), (6, 1, 0), (0, 0, 3), (0, 0, 5), (1, 2, 7),
    (5, 7, 0), (5, 7, 1), (1, 2, 2), (1, 0, 3), (1, 0, 5), (1, 2, 6), (4, 0, 0), (0, 2, 2), (0, 2, 6), (5, 2, 0),
    (5, 2, 1), (5, 6, 0), (5, 6, 1), (6, 7, 0), (0, 1, 3), (0, 1, 5), (1, 1, 3), (1, 3, 3), (0, 3, 3), (0, 3, 5),
    (3, 0, 7), (1, 1, 5), (1, 3, 5), (6, 2, 0), (0, 0, 4), (2, 1, 0), (2, 3, 0), (6, 6, 0), (7, 1, 0), (0, 2, 5),
    (7, 1, 1), (7, 7, 0), (1, 2, 3), (7, 7, 1), (3, 0, 6), (1, 0, 4), (3, 0, 1), (1, 2, 5), (5, 5, 0), (2, 2, 0),
    (5, 5, 1), (0, 2, 3), (5, 3, 0), (5, 3, 1), (3, 0, 5), (7, 2, 0), (0, 1, 4), (7, 2, 1), (7, 6, 0), (7, 6, 1),
    (0, 3, 4), (3, 0, 2), (1, 1, 4), (1, 3, 4), (4, 1, 0), (0, 2, 4), (6, 5, 0), (3, 0, 3), (2, 0, 7), (6, 3, 0),
    (3, 3, 0), (2, 0, 1), (2, 1, 7), (2, 1, 1), (3, 3, 1), (2, 2, 7), (1, 2, 4), (2, 2, 1), (5, 4, 0), (2, 3, 7),
    (3, 3, 2), (2, 3, 1), (5, 4, 1), (3, 1, 0), (2, 0, 6), (3, 3, 5), (2, 1, 6), (3, 0, 4), (3, 1, 1), (3, 3, 6),
    (2, 2, 6), (2, 0, 2), (7, 3, 0), (3, 1, 2), (7, 3, 1), (2, 3, 6), (2, 1, 2), (3, 3, 7), (7, 5, 0), (2, 2, 2),
    (2, 0, 5), (3, 1, 5), (7, 5, 1), (3, 3, 3), (2, 3, 2), (2, 1, 5), (3, 1, 6), (2, 0, 3), (2, 2, 5), (3, 3, 4),
    (3, 1, 7), (6, 4, 0), (2, 1, 3), (2, 3, 5), (3, 1, 3), (2, 2, 3), (3, 2, 0), (2, 3, 3), (3, 1, 4), (2, 0, 4),
    (3, 2, 1), (8, 0, 0), (2, 1, 4), (3, 2, 2), (2, 2, 4), (3, 2, 5), (8, 0, 1), (2, 3, 4), (3, 2, 6), (3, 2, 7),
    (7, 4, 0), (3, 2, 3), (7, 4, 1), (3, 2, 4), (10, 0, 0), (8, 2, 0), (8, 1, 0), (8, 1, 1), (8, 2, 1), (8, 3, 0),
    (8, 3, 1), (8, 4, 0), (8, 4, 1), (8, 5, 0), (8, 5, 1), (8, 6, 0), (8, 6, 1), (8, 7, 0), (8, 7, 1),
)


def kernel(pair, res, coef, slots, ct, grouped, blocks, weights, stage, coefs, wide, parts, other, final, gamma, total,
           column, own_coef, own_slots, load_sem, block_sem, coef_sem, send_sem, half_sem,
           plane_sem):
    row, x = lax.axis_index("rows"), lax.axis_index("panel")
    core, y, z = row % NC, (row // NC) % NY, row // (NC * NY)
    turn = 1 - 2 * core
    mate = row + turn
    bf16, f32 = jnp.bfloat16, jnp.float32

    def at(dy, dz):
        return (y + NY - turn * dy) % NY, (z + NZ - turn * dz) % NZ

    def device(dy, dz):
        ty, tz = (y + NY + turn * dy) % NY, (z + NZ + turn * dz) % NZ
        return ((tz * NY + ty) * NC + core, x)

    def remote(src, dst, sent, got, to):
        return pltpu.make_async_remote_copy(
            src_ref=src, dst_ref=dst, send_sem=sent, recv_sem=got, device_id=to, device_id_type=MESH
        )

    own = z * NY + y
    step = KB // 4
    load_pair = pltpu.make_async_copy(pair, blocks.at[own], load_sem.at[4])
    load_pair.start()
    loads = [
        pltpu.make_async_copy(res.at[pl.ds(i * step, step)], stage.at[pl.ds(i * step, step)], load_sem.at[i])
        for i in range(4)
    ]
    load_coef = pltpu.make_async_copy(coef, own_coef, load_sem.at[5])
    load_slots = pltpu.make_async_copy(slots, own_slots, load_sem.at[6])
    for load in loads + [load_coef, load_slots]:
        load.start()

    barrier = pltpu.get_barrier_semaphore()
    peers = [device(1, 0), device(-1, 0), device(0, 1), device(0, -1), (mate, x)]
    peers += [(r, (x + d) % NX) for d in range(1, NX) for r in (row, mate)]
    for peer in peers:
        pl.semaphore_signal(barrier, inc=1, device_id=peer, device_id_type=MESH)
    load_pair.wait()
    pl.semaphore_wait(barrier, len(peers))

    def piece(kind, place):
        chip = place[1] * NY + place[0]
        if kind < 2:
            return blocks.at[chip, :, pl.ds(0, KA) if kind == 0 else pl.ds(KA, KB - KA)]
        return coefs.at[chip * NC + core, :, pl.ds(0, CA) if kind == 2 else pl.ds(CA, CP - CA)]

    def arrival(kind, place):
        sems = block_sem if kind < 2 else coef_sem
        return sems.at[kind % 2, place[1] * NY + place[0]]

    held = []
    opened = []

    def pass_on(kind, dy, dz):
        place = at(dy, dz)
        ref = piece(kind, place)
        along_y = []
        along_z = []
        if kind % 2 == 0:
            if dz == 0:
                along_y = [1] * (dy in (0, 1)) + [-1] * (dy == 0)
                along_z = [1, -1]
            else:
                along_z = [1] * (dz in (1, 2, 3)) + [-1] * (dz in (6, 7))
        else:
            if dy == 0:
                along_z = [1] * (dz in (0, 1, 2, 3)) + [-1] * (dz in (0, 6, 7))
                along_y = [1, -1]
            elif dy == 1:
                along_y = [1]
        for hop in [(d, 0) for d in along_y] + [(0, d) for d in along_z]:
            copy = remote(ref, ref, send_sem.at[kind], arrival(kind, place), device(*hop))
            second = (kind == 2 and dz == 0 and hop[0] == 0) or (kind == 3 and dy == 0 and hop[1] == 0)
            if second and not opened:
                held.append((kind, dy + dz, len(held), copy))
            else:
                copy.start()

    def share_coefs(place):
        ref = coefs.at[(place[1] * NY + place[0]) * NC + core]
        remote(ref, ref, send_sem.at[4], plane_sem.at[2, place[1]], (mate, x)).start()

    whole = weights.at[1 - core]

    def prepare(i, _):
        if i < 4:
            loads[i].wait()
            weights[core, pl.ds(i * step, step), :] = stage[pl.ds(i * step, step), :].astype(bf16)
        if 0 < i < 5:
            ref = weights.at[core, pl.ds((i - 1) * step, step)]
            remote(ref, ref, half_sem.at[0], half_sem.at[1], (mate, x)).start()
        if i == 5:
            load_coef.wait()
            coefs[row] = jnp.concatenate([own_coef[...], jnp.zeros((CR, CP - CM), bf16)], axis=1)
            load_slots.wait()
            for j in range(16):
                wide_row = jnp.broadcast_to(own_slots[j : j + 1, :].astype(f32), (128, 128))
                column[pl.ds(j * 128, 128), :] = jnp.transpose(wide_row).astype(jnp.int32)

    multiplied = set()

    def multiply(dz, half):
        if not multiplied:
            remote(whole, whole, half_sem.at[0], half_sem.at[1], (mate, x)).wait_recv()
        multiplied.add((dz, half))
        _, plane = at(0, dz)
        left = blocks[pl.ds(plane * NY, NY)].reshape(NY * ROWS, KB)
        prod = jnp.dot(left, weights[half], preferred_element_type=f32).reshape(NY, ROWS, PB)
        wide[plane, :, half] = prod
        parts[plane, :, half] = prod.astype(bf16)
        if half == NC - 1:
            for d in range(1, NX):
                to = (x + d) % NX
                ref = other.at[plane, d - 1]
                remote(parts.at[plane, to], ref, send_sem.at[5], plane_sem.at[0, plane], (row, to)).start()

    def add_up(dz, _):
        _, plane = at(0, dz)
        ref = other.at[plane]
        remote(ref, ref, send_sem.at[5], plane_sem.at[0, plane], (row, x)).wait_recv()
        value = wide[plane, x]
        for d in range(NX - 1):
            value = value + other[plane, d].astype(f32)
        final[plane] = value.astype(bf16)
        spot = plane * (NY * NC) + x * NC + core
        gamma[spot] = final[plane, core]
        remote(final.at[plane, 1 - core], gamma.at[spot], send_sem.at[6], plane_sem.at[1, plane], (mate, x)).start()
        for d in range(1, NX):
            for c in range(NC):
                to = ((z * NY + y) * NC + c, (x + d) % NX)
                remote(final.at[plane, c], gamma.at[spot], send_sem.at[6], plane_sem.at[1, plane], to).start()

    selected = set()

    def select(dz, part):
        _, plane = at(0, dz)
        if part == 0:
            ref = gamma.at[pl.ds(0, NY * NC - 1)]
            remote(ref, ref, send_sem.at[6], plane_sem.at[1, plane], (mate, x)).wait_recv()
        rows = gamma[pl.ds(plane * (NY * NC), NY * NC)].reshape(NY * NC * ROWS, PB)
        lanes = lax.broadcasted_iota(jnp.int32, (1024, 128), 1)
        at_rows = pl.ds(part * 1024, 1024)
        ids = column[at_rows, :] - plane * (NY * NC * ROWS)
        pick = jnp.concatenate(
            [jnp.where(ids == lanes + h * 128, 1.0, 0.0).astype(bf16) for h in range(2)], axis=1
        )
        found = jnp.dot(pick, rows, preferred_element_type=f32)
        if part in selected:
            found = total[at_rows, :] + found
        selected.add(part)
        total[at_rows, :] = found

    def transpose(dz, part):
        _, plane = at(0, dz)
        if part == 0:
            ref = coefs.at[pl.ds(0, NY)]
            remote(ref, ref, send_sem.at[4], plane_sem.at[2, plane], (mate, x)).wait_recv()
        cols = pl.ds(part * 1408, 1408)
        tile = coefs[pl.ds(plane * (NY * NC), NY * NC), :, cols].reshape(128, 1408)
        ct[plane, cols] = jnp.transpose(tile)

    def deliver(_, __):
        grouped[...] = total[...].astype(bf16)

    pass_on(0, 0, 0)
    pass_on(1, 0, 0)
    seen = {}
    for kind, dy, dz in ORDER:
        if kind < 4:
            place = at(dy, dz)
            ref = piece(kind, place)
            remote(ref, ref, send_sem.at[kind], arrival(kind, place), (mate, x)).wait_recv()
            pass_on(kind, dy, dz)
            if kind >= 2:
                seen[dy, dz] = seen.get((dy, dz), 0) + 1
                if seen[dy, dz] == 2:
                    share_coefs(place)
        elif kind == 4 and dy == 1:
            for entry in sorted(held, key=lambda entry: entry[:3]):
                entry[3].start()
            opened.append(True)
        elif kind == 4:
            pass_on(3, 0, 0)
            pass_on(2, 0, 0)
            share_coefs(at(0, 0))
        else:
            {5: multiply, 6: add_up, 7: select, 8: transpose, 9: prepare, 10: deliver}[kind](dy, dz)

    def drained(ref, sem):
        remote(ref, ref, sem, half_sem.at[1], (mate, x)).wait_send()

    sends = NY * NZ - 1
    drained(blocks.at[pl.ds(0, sends), :, pl.ds(0, KA)], send_sem.at[0])
    drained(blocks.at[pl.ds(0, sends), :, pl.ds(KA, KB - KA)], send_sem.at[1])
    drained(coefs.at[pl.ds(0, sends), :, pl.ds(0, CA)], send_sem.at[2])
    drained(coefs.at[pl.ds(0, sends), :, pl.ds(CA, CP - CA)], send_sem.at[3])
    drained(coefs.at[pl.ds(0, NY * NZ)], send_sem.at[4])
    drained(other, send_sem.at[5])
    drained(gamma.at[pl.ds(0, NZ * (NY * NC - 1))], send_sem.at[6])
    drained(whole, half_sem.at[0])


def finish(ct, grouped, out, result, result_sem):
    tall = CM // CHUNKS
    half = NZ * NY * NC * CR
    puts = []
    for i in range(CHUNKS):
        rows = pl.ds(i * tall, tall)
        tile = jnp.concatenate([ct[plane, rows] for plane in range(NZ)], axis=1)
        for o in range(2):
            result[o, rows] = jnp.dot(tile, grouped[pl.ds(o * half, half)], preferred_element_type=jnp.float32)
        puts.append(pltpu.make_async_copy(result.at[:, rows], out.at[:, rows], result_sem.at[i]))
        puts[i].start()
    for put in puts:
        put.wait()


def body(pair_block, resolvent, virt_coef, slot_row):
    dma = pltpu.SemaphoreType.DMA
    bf16, f32 = jnp.bfloat16, jnp.float32
    anywhere = pl.BlockSpec(memory_space=pl.ANY)
    vmem = pl.BlockSpec(memory_space=pltpu.VMEM)
    given = (pair_block, resolvent, virt_coef, slot_row.reshape(16, 128))
    width = NY * NC * CR
    tall = NZ * NY * NC * ROWS
    ct, grouped = pl.pallas_call(
        kernel,
        out_shape=(jax.ShapeDtypeStruct((NZ, CP, width), bf16), jax.ShapeDtypeStruct((tall, PB), bf16)),
        in_specs=[anywhere] * 4,
        out_specs=(vmem, vmem),
        scratch_shapes=[
            pltpu.VMEM((NY * NZ, ROWS, KB), bf16),
            pltpu.VMEM((NC, KB, PB), bf16),
            pltpu.VMEM((KB, PB), f32),
            pltpu.VMEM((NY * NZ * NC, CR, CP), bf16),
            pltpu.VMEM((NZ, NY, NC, ROWS, PB), f32),
            pltpu.VMEM((NZ, NY, NC, ROWS, PB), bf16),
            pltpu.VMEM((NZ, NX - 1, NC, ROWS, PB), bf16),
            pltpu.VMEM((NZ, NC, ROWS, PB), bf16),
            pltpu.VMEM((NZ * NY * NC, ROWS, PB), bf16),
            pltpu.VMEM((tall, PB), f32),
            pltpu.VMEM((tall, 128), jnp.int32),
            pltpu.VMEM((CR, CM), bf16),
            pltpu.VMEM((16, 128), jnp.int32),
            dma((7,)),
            dma((2, NY * NZ)),
            dma((2, NY * NZ)),
            dma((7,)),
            dma((2,)),
            dma((3, NZ)),
        ],
        compiler_params=pltpu.CompilerParams(
            collective_id=0, has_side_effects=True, vmem_limit_bytes=40 * 1024 * 1024
        ),
    )(*(pltpu.with_memory_space_constraint(a, pltpu.HBM) for a in given))
    return pl.pallas_call(
        finish,
        out_shape=jax.ShapeDtypeStruct((2, CM, PB), f32),
        in_specs=[vmem, vmem],
        out_specs=anywhere,
        scratch_shapes=[
            pltpu.VMEM((2, CM, PB), f32),
            dma((CHUNKS,)),
        ],
        compiler_params=pltpu.CompilerParams(vmem_limit_bytes=16 * 1024 * 1024),
        cost_estimate=pl.CostEstimate(flops=4 * CM * NZ * width * PB, bytes_accessed=12000000, transcendentals=0),
    )(ct, grouped)


def solution(mesh):
    placed = (P("rows", "panel"), P("panel", "rows"), P("rows", "panel"), P())
    return jax.shard_map(
        body, mesh=mesh, in_specs=placed, out_specs=P(None, "panel", "rows"), check_vma=False
    )
```
